32 devices in a mesh: lb: 4 (over z), rb: 4 (over y, x), wa: 2 (over core).
Axes of the slice: x: 2, y: 2, z: 4, core: 2. Of those that a mesh axis runs over, the one named last changes fastest.
Arguments:
- initial_guess: bfloat16 [8192, 4, 128], P(('lb', 'rb')), may hold values from -6 to 6
- left_environment: bfloat16 [8, 4, 4, 512, 8192], P('wa', None, 'rb', None, 'lb'), may hold values from -12 to 12, as said below
- right_environment: bfloat16 [128, 8, 128], replicated, may hold values from -12 to 12, as said below
- operator_blocks: float32 [16, 4, 4], replicated, may hold values from -4 to 4
- operator_pairs: int32 [16, 2], replicated, may hold values from 0 to 7
Outputs:
- ritz_vector: float32 [8192, 4, 128], P(('lb', 'rb'))
- residual: float32 [8192, 4, 128], P(('lb', 'rb'))
The draws below stay inside these ranges and needn't reach their ends.
Inputs may be any that keep to these rules, and one draw needn't show every extreme that they name: `operator_pairs`: each row names the left and the right MPO index of one operator block; blocks with the same pair add. `left_environment`: for each MPO index the [8192, 8192] matrix is symmetric. `right_environment`: for each MPO index the matrix over the two right bond states is symmetric.
All inputs are finite; a program needn't handle non-finite values.
Results may differ from the reference program's by a relative error of at most 0.014.
Values may be sent and summed in bfloat16 or wider, within the bound.
A program may use at most 192 MiB of HBM per device.

```python
import jax
import jax.numpy as jnp
from jax import lax

DL = 8192
RB = 128
W = 8
NB = 16
ITERS = 3
SWEEPS = 8
S = 4
N_LB = 4
N_RB = 4


def draw_left_environment(key, part):
    noise_key = jax.random.fold_in(key, 11)
    scale_key = jax.random.fold_in(key, 12)
    noise = jax.random.normal(noise_key, (W, DL, DL), jnp.float32)
    symmetric = (noise + jnp.swapaxes(noise, 1, 2)) * (0.5 / jnp.sqrt(DL * 1.0))
    scales = jnp.exp(jax.random.uniform(scale_key, (W, DL), jnp.float32, 0.0, 2.0))
    positions = jnp.arange(DL, dtype=jnp.int32)
    symmetric = symmetric.at[:, positions, positions].add(scales)
    return symmetric.reshape(W, N_LB, N_RB, DL // (N_LB * N_RB), DL).astype(jnp.bfloat16)


def draw_right_environment(key, part):
    noise_key = jax.random.fold_in(key, 21)
    scale_key = jax.random.fold_in(key, 22)
    noise = jax.random.normal(noise_key, (RB, W, RB), jnp.float32)
    symmetric = (noise + jnp.transpose(noise, (2, 1, 0))) * (0.5 / jnp.sqrt(RB * 1.0))
    scales = jnp.exp(jax.random.uniform(scale_key, (W, RB), jnp.float32, 0.0, 2.0))
    symmetric = symmetric + jnp.eye(RB, dtype=jnp.float32)[:, None, :] * scales[None, :, :]
    return symmetric.astype(jnp.bfloat16)


def place_ends(entries, rng, least, top_value):
    shape = entries.shape
    place = [jax.random.randint(jax.random.fold_in(rng, axis), (), 0, shape[axis]) for axis in range(len(shape))]
    entries = entries.at[tuple(place)].set(least)
    longest = shape.index(max(shape))
    place[longest] = (place[longest] + 1) % shape[longest]
    return entries.at[tuple(place)].set(top_value)


def block_scale(key, dims, split, smallest, high):
    loudness, own = 1.0, jax.random.fold_in(key, 6)
    for axis_at, parts in split:
        draws = jnp.exp(jax.random.uniform(jax.random.fold_in(own, axis_at), (parts,), jnp.float32, smallest / len(split), high / len(split)))
        loudness = loudness * jnp.repeat(draws, dims[axis_at] // parts).reshape([-1 if axis == axis_at else 1 for axis in range(len(dims))])
    return loudness


def scatter_about(key, extent, deviation, reach, shards=(), kind=jnp.bfloat16):
    values = deviation * jax.random.normal(key, extent, jnp.float32)
    if shards:
        values = values * block_scale(key, extent, shards, -0.22, 0.18)
    return jnp.clip(values, -reach, reach).astype(kind)


def setup_inputs(seed: int = 0) -> dict:
    key_list = jax.random.split(jax.random.key(seed), 6)
    initial_guess = scatter_about(key_list[0], (DL, S, RB), 1.0, 6.0, ((0, 16),))
    left_environment = draw_left_environment(jax.random.fold_in(key_list[5], 71), 0)
    right_environment = draw_right_environment(jax.random.fold_in(key_list[5], 71), 0)
    operator_blocks = scatter_about(key_list[3], (NB, S, S), 0.3, 4.0, (), jnp.float32)
    operator_pairs = place_ends(jax.random.randint(key_list[4], (NB, 2), 0, W), jax.random.fold_in(key_list[4], 1), 0, W - 1).astype(jnp.int32)
    return dict(initial_guess=initial_guess, left_environment=left_environment, right_environment=right_environment, operator_blocks=operator_blocks, operator_pairs=operator_pairs)


highest = lax.Precision.HIGHEST
epsilon = 1e-06

def lowest_pair(matrix):
    matrix_order = matrix.shape[0]
    vectors = jnp.eye(matrix_order, dtype=jnp.float32)
    for rounds in range(SWEEPS):
        for first_row in range(matrix_order):
            for second_row in range(first_row + 1, matrix_order):
                rotation_angle = 0.5 * jnp.arctan2(2.0 * matrix[first_row, second_row], matrix[second_row, second_row] - matrix[first_row, first_row])
                cosine = jnp.cos(rotation_angle)
                sine_value = jnp.sin(rotation_angle)
                rotation = jnp.eye(matrix_order, dtype=jnp.float32)
                rotation = rotation.at[first_row, first_row].set(cosine).at[second_row, second_row].set(cosine)
                rotation = rotation.at[first_row, second_row].set(sine_value).at[second_row, first_row].set(-sine_value)
                matrix = jnp.dot(rotation.T, jnp.dot(matrix, rotation, precision=highest), precision=highest)
                vectors = jnp.dot(vectors, rotation, precision=highest)
    values = jnp.diagonal(matrix)
    chosen = (jnp.arange(matrix_order, dtype=jnp.int32) == jnp.argmin(values).astype(jnp.int32)).astype(jnp.float32)
    ritz_value = jnp.sum(values * chosen)
    weights = jnp.dot(vectors, chosen, precision=highest)
    weights = jnp.where(weights[0] < 0.0, -weights, weights)
    return (ritz_value, weights)

def dense_operator(operator_blocks, operator_pairs, levels):
    symmetric = 0.5 * (operator_blocks + jnp.swapaxes(operator_blocks, 1, 2))
    indices = jnp.arange(levels, dtype=jnp.int32)
    left_hot = (operator_pairs[:, 0:1] == indices[None, :]).astype(jnp.float32)
    right_hot = (operator_pairs[:, 1:2] == indices[None, :]).astype(jnp.float32)
    return jnp.einsum('nw,nv,nts->wvts', left_hot, right_hot, symmetric, precision=highest)

def contract_right(vector_rows, right_matrix, local_operator):
    row_count, physical, window = vector_rows.shape
    levels = local_operator.shape[1]
    mixed = jnp.dot(vector_rows.reshape(row_count * physical, window), right_matrix, preferred_element_type=jnp.float32)
    mixed = mixed.reshape(row_count, physical, levels, window)
    return jnp.einsum('kvts,nsvb->kntb', local_operator, mixed, precision=highest).astype(jnp.bfloat16)

def combine(members, weights):
    total = weights[0] * members[0]
    for member_index in range(1, len(members)):
        total = total + weights[member_index] * members[member_index]
    return total

def reference(initial_guess, left_environment, right_environment, operator_blocks, operator_pairs):
    total_count = DL * S * RB
    left_matrix = left_environment.reshape(W, DL, DL)
    right_matrix = right_environment.reshape(RB, W * RB)
    operator = dense_operator(operator_blocks, operator_pairs, W)

    def apply_hamiltonian(vector):
        inner_terms = contract_right(vector.astype(jnp.bfloat16), right_matrix, operator)
        flat = inner_terms.reshape(W, DL, S * RB)
        image = jnp.zeros((DL, S * RB), jnp.float32)
        for level in range(W):
            image = image + jnp.dot(left_matrix[level], flat[level], preferred_element_type=jnp.float32)
        return image.reshape(DL, S, RB)

    def mean_product(first_array, second_array):
        return jnp.sum(first_array * second_array) / total_count
    left_diag = jnp.diagonal(left_matrix, axis1=1, axis2=2).astype(jnp.float32)
    operator_diag = jnp.diagonal(operator, axis1=2, axis2=3)
    right_diag = jnp.diagonal(right_environment, axis1=0, axis2=2).astype(jnp.float32)
    diagonal_values = jnp.einsum('ka,kvs,vb->asb', left_diag, operator_diag, right_diag, precision=highest)
    start_vector = initial_guess.astype(jnp.float32)
    basis = [start_vector * lax.rsqrt(mean_product(start_vector, start_vector) + epsilon)]
    images = [apply_hamiltonian(basis[0])]
    subspace = jnp.zeros((ITERS + 1, ITERS + 1), jnp.float32)
    subspace = subspace.at[0, 0].set(mean_product(basis[0], images[0]))
    for step_index in range(ITERS):
        filled = step_index + 1
        ritz_value, weights = lowest_pair(subspace[:filled, :filled])
        ritz_now = combine(basis, weights)
        residual_now = combine(images, weights) - ritz_value * ritz_now
        correction = residual_now / (jnp.abs(diagonal_values - ritz_value) + 1.0)
        correlations = jnp.stack([mean_product(member, correction) for member in basis])
        correction = correction - combine(basis, correlations)
        new_vector = correction * lax.rsqrt(mean_product(correction, correction) + epsilon)
        new_image = apply_hamiltonian(new_vector)
        basis.append(new_vector)
        images.append(new_image)
        row_values = jnp.stack([mean_product(member, new_image) for member in basis])
        subspace = subspace.at[filled, :filled + 1].set(row_values).at[:filled + 1, filled].set(row_values)
    ritz_value, weights = lowest_pair(subspace)
    ritz_vector = combine(basis, weights)
    residual = combine(images, weights) - ritz_value * ritz_vector
    return (ritz_vector, residual)
```

```python
import functools

import jax
import jax.numpy as jnp
from jax import lax
from jax.experimental import pallas as pl
from jax.experimental.pallas import tpu as pltpu
from jax.sharding import PartitionSpec as P

ITERS = 3
SWEEPS = 8

highest = lax.Precision.HIGHEST
epsilon = 1e-06


TILE = (8, 128)


def half_angle(y, x):
    scale = jnp.maximum(jnp.abs(x), jnp.abs(y))
    zero = scale == 0.0
    inverse = 1.0 / jnp.where(zero, 1.0, scale)
    xs, ys = x * inverse, y * inverse
    h = jnp.sqrt(xs * xs + ys * ys)
    h = jnp.where(zero, 1.0, h)
    big = jnp.sqrt(0.5 * (1.0 + jnp.abs(xs) / h))
    small = 0.5 * jnp.abs(ys) / (h * big)
    positive = x >= 0.0
    cosine = jnp.where(positive, big, small)
    sine = jnp.where(positive, small, big) * jnp.where(y < 0.0, -1.0, 1.0)
    return jnp.where(zero, 1.0, cosine), jnp.where(zero, 0.0, sine)


def jacobi_kernel(order, entries_ref, out_ref):
    def at(i, j):
        return (min(i, j), max(i, j))

    keys = [(i, j) for i in range(order) for j in range(i, order)]
    start = tuple(
        jnp.full(TILE, entries_ref[i, j], jnp.float32) for i, j in keys
    )
    one, none = jnp.full(TILE, 1.0, jnp.float32), jnp.full(TILE, 0.0, jnp.float32)
    vectors0 = tuple(
        one if i == j else none for i in range(order) for j in range(order)
    )

    def sweep(_, carry):
        m = dict(zip(keys, carry[0]))
        v = list(carry[1])
        for p in range(order):
            for q in range(p + 1, order):
                a, b, d = m[(p, p)], m[(p, q)], m[(q, q)]
                c, s = half_angle(2.0 * b, d - a)
                m[(p, p)] = c * (c * a - s * b) - s * (c * b - s * d)
                m[(p, q)] = s * (c * a - s * b) + c * (c * b - s * d)
                m[(q, q)] = s * (s * a + c * b) + c * (s * b + c * d)
                for i in range(order):
                    if i != p and i != q:
                        x, y = m[at(i, p)], m[at(i, q)]
                        m[at(i, p)] = c * x - s * y
                        m[at(i, q)] = s * x + c * y
                    x, y = v[i * order + p], v[i * order + q]
                    v[i * order + p] = c * x - s * y
                    v[i * order + q] = s * x + c * y
        return tuple(m[key] for key in keys), tuple(v)

    values, vectors = lax.fori_loop(0, SWEEPS, sweep, (start, vectors0))
    m = dict(zip(keys, values))
    best = m[(0, 0)]
    weights = [vectors[i * order] for i in range(order)]
    for j in range(1, order):
        better = m[(j, j)] < best
        best = jnp.where(better, m[(j, j)], best)
        weights = [
            jnp.where(better, vectors[i * order + j], weights[i]) for i in range(order)
        ]
    sign = jnp.where(weights[0] < 0.0, -1.0, 1.0)
    out_ref[0] = best
    for i in range(order):
        out_ref[i + 1] = weights[i] * sign


def lowest_pair(matrix):
    order = matrix.shape[0]
    if order == 1:
        return matrix[0, 0], jnp.ones((1,), jnp.float32)
    found = pl.pallas_call(
        functools.partial(jacobi_kernel, order),
        out_shape=jax.ShapeDtypeStruct((order + 1,) + TILE, jnp.float32),
        in_specs=[pl.BlockSpec(memory_space=pltpu.SMEM)],
        out_specs=pl.BlockSpec(memory_space=pltpu.VMEM),
    )(matrix)
    flat = found[:, 0, 0]
    return flat[0], flat[1:]


def dense_operator(operator_blocks, operator_pairs, levels):
    symmetric = 0.5 * (operator_blocks + jnp.swapaxes(operator_blocks, 1, 2))
    indices = jnp.arange(levels, dtype=jnp.int32)
    left_hot = (operator_pairs[:, 0:1] == indices[None, :]).astype(jnp.float32)
    right_hot = (operator_pairs[:, 1:2] == indices[None, :]).astype(jnp.float32)
    return jnp.einsum("nw,nv,nts->wvts", left_hot, right_hot, symmetric, precision=highest)


def combine(members, weights):
    total = weights[0] * members[0]
    for member_index in range(1, len(members)):
        total = total + weights[member_index] * members[member_index]
    return total


def shifted(part, axis, step):
    size = lax.axis_size(axis)
    return lax.ppermute(part, axis, [(i, (i + step) % size) for i in range(size)])


def gather_axis(part, axis):
    size = lax.axis_size(axis)
    index = lax.axis_index(axis)
    whole = jnp.zeros((size,) + part.shape, part.dtype)
    for step in range(size):
        piece = shifted(part, axis, step) if step else part
        source = lax.rem(index - step + size, size)
        whole = lax.dynamic_update_index_in_dim(whole, piece, source, 0)
    return whole


def gather_rows(part):
    rb_size, wa_size = lax.axis_size("rb"), lax.axis_size("wa")
    rb_index, wa_index = lax.axis_index("rb"), lax.axis_index("wa")
    whole = jnp.zeros((rb_size, wa_size) + part.shape, part.dtype)
    for step in range(rb_size):
        piece = shifted(part, "rb", step) if step else part
        rb_source = lax.rem(rb_index - step + rb_size, rb_size)
        for turn in range(wa_size):
            own = shifted(piece, "wa", turn) if turn else piece
            wa_source = lax.rem(wa_index - turn + wa_size, wa_size)
            whole = lax.dynamic_update_slice(
                whole, own[None, None], (rb_source, wa_source, 0, 0)
            )
    return whole.reshape(rb_size * wa_size * part.shape[0], part.shape[1])


def sum_everywhere(total):
    for axis in ("lb", "rb", "wa"):
        size = lax.axis_size(axis)
        if size & (size - 1):
            total = lax.psum(total, axis)
            continue
        stride = 1
        while stride < size:
            total = total + lax.ppermute(total, axis, [(i, i ^ stride) for i in range(size)])
            stride *= 2
    return total


def per_device(initial_guess, left_environment, right_environment, operator_blocks, operator_pairs):
    own_rows, physical, window = initial_guess.shape
    width = physical * window
    levels = right_environment.shape[1]
    local_levels = left_environment.shape[0]
    coarse = left_environment.shape[1]
    block_rows = coarse * left_environment.shape[3]
    contracted = left_environment.shape[4]
    lb_size, rb_size, wa_size = lax.axis_size("lb"), lax.axis_size("rb"), lax.axis_size("wa")
    half_rows = own_rows // wa_size
    total_count = own_rows * physical * window * lb_size * rb_size
    left_index = lax.axis_index("lb")
    right_index = lax.axis_index("rb")
    level_index = lax.axis_index("wa")

    operator = dense_operator(operator_blocks, operator_pairs, levels)
    local_operator = lax.dynamic_slice_in_dim(operator, level_index * local_levels, local_levels, 0)
    left_matrix = left_environment.reshape(local_levels, block_rows, contracted)

    joint = jnp.einsum(
        "kvts,cvb->ksctb",
        local_operator,
        right_environment.astype(jnp.float32),
        precision=highest,
    ).reshape(local_levels, width, width)
    joint_high = joint.astype(jnp.bfloat16)
    joint_low = (joint - joint_high.astype(jnp.float32)).astype(jnp.bfloat16)
    joint_matrix = jnp.concatenate([joint_high, joint_low], axis=1)

    own_block = lax.dynamic_slice(
        left_environment,
        (0, left_index, 0, 0, right_index * own_rows),
        (local_levels, 1, 1, own_rows, own_rows),
    ).reshape(local_levels, own_rows, own_rows)
    same = lax.broadcasted_iota(jnp.int32, (own_rows, own_rows), 0) == lax.broadcasted_iota(
        jnp.int32, (own_rows, own_rows), 1
    )
    left_diag = jnp.sum(
        jnp.where(same[None], own_block.astype(jnp.float32), 0.0), axis=2
    )
    left_diag = gather_axis(left_diag, "wa").reshape(levels, own_rows)
    left_diag = lax.dynamic_slice_in_dim(left_diag, level_index * half_rows, half_rows, 1)
    operator_diag = jnp.diagonal(operator, axis1=2, axis2=3)
    right_diag = jnp.diagonal(right_environment, axis1=0, axis2=2).astype(jnp.float32)
    level_rows = jnp.einsum("kvs,vb->ksb", operator_diag, right_diag, precision=highest)
    diagonal_values = jnp.dot(
        left_diag.T, level_rows.reshape(levels, width), precision=highest
    )

    def apply_hamiltonian(vector_bf):
        rows = gather_rows(vector_bf)
        doubled = jnp.concatenate([rows, rows], axis=1)
        inner_terms = jnp.einsum(
            "np,kpq->knq", doubled, joint_matrix, preferred_element_type=jnp.float32
        ).astype(jnp.bfloat16)
        partial_value = jnp.einsum(
            "kma,kaq->mq", left_matrix, inner_terms, preferred_element_type=jnp.float32
        ).reshape(coarse, wa_size, half_rows, width)
        kept = lax.dynamic_index_in_dim(partial_value, level_index, 1, keepdims=False)
        for step in range(1, wa_size):
            target = lax.rem(level_index + step, wa_size)
            sent = lax.dynamic_index_in_dim(partial_value, target, 1, keepdims=False)
            ring = [(i, (i + step) % wa_size) for i in range(wa_size)]
            kept = kept + lax.ppermute(sent.astype(jnp.bfloat16), "wa", ring).astype(jnp.float32)
        image = lax.dynamic_index_in_dim(kept, left_index, 0, keepdims=False)
        for step in range(1, lb_size):
            target = lax.rem(left_index + step, lb_size)
            sent = lax.dynamic_index_in_dim(kept, target, 0, keepdims=False)
            ring = [(i, (i + step) % lb_size) for i in range(lb_size)]
            image = image + lax.ppermute(sent.astype(jnp.bfloat16), "lb", ring).astype(jnp.float32)
        return image

    def mean_products(pairs):
        local = jnp.stack([jnp.sum(first * second) for first, second in pairs])
        return sum_everywhere(local) / total_count

    guess = lax.dynamic_slice_in_dim(initial_guess, level_index * half_rows, half_rows, 0)
    guess = guess.reshape(half_rows, width)
    start_vector = guess.astype(jnp.float32)
    raw_image = apply_hamiltonian(guess)
    sums = mean_products([(start_vector, start_vector), (start_vector, raw_image)])
    scale = lax.rsqrt(sums[0] + epsilon)
    basis = [start_vector * scale]
    images = [raw_image * scale]
    subspace = (sums[1] * scale * scale).reshape(1, 1)
    for step_index in range(ITERS):
        filled = step_index + 1
        ritz_value, weights = lowest_pair(subspace)
        ritz_now = combine(basis, weights)
        residual_now = combine(images, weights) - ritz_value * ritz_now
        correction = residual_now / (jnp.abs(diagonal_values - ritz_value) + 1.0)
        correlation_values = mean_products([(member, correction) for member in basis])
        correction = correction - combine(basis, correlation_values)
        raw_image = apply_hamiltonian(correction.astype(jnp.bfloat16))
        sums = mean_products(
            [(correction, correction)]
            + [(member, raw_image) for member in basis]
            + [(correction, raw_image)]
        )
        scale = lax.rsqrt(sums[0] + epsilon)
        basis.append(correction * scale)
        images.append(raw_image * scale)
        row = sums[1 : filled + 1] * scale
        corner = (sums[filled + 1] * scale * scale).reshape(1, 1)
        subspace = jnp.concatenate(
            [
                jnp.concatenate([subspace, row[:, None]], axis=1),
                jnp.concatenate([row[None, :], corner], axis=1),
            ],
            axis=0,
        )
    ritz_value, weights = lowest_pair(subspace)
    ritz_vector = combine(basis, weights)
    residual = combine(images, weights) - ritz_value * ritz_vector

    def whole_rows(part):
        whole = gather_axis(part, "wa")
        return whole.reshape(own_rows, physical, window)

    return whole_rows(ritz_vector), whole_rows(residual)


def solution(mesh):
    in_specs = (P(("lb", "rb"), None, None), P("wa", None, "rb", None, "lb"), P(), P(), P())
    out_specs = (P(("lb", "rb"), None, None), P(("lb", "rb"), None, None))
    return jax.shard_map(
        per_device, mesh=mesh, in_specs=in_specs, out_specs=out_specs, check_vma=False
    )
```
